32 devices in a mesh: member: 4 (over y, core), mesh: 8 (over z, x).
Axes of the slice: x: 2, y: 2, z: 4, core: 2. Of those that a mesh axis runs over, the one named last changes fastest.
Arguments:
- hidden_embedding: bfloat16 [8, 4096, 512], P('member', 'mesh'), may hold values from -6 to 6
- decoder_matrix: bfloat16 [512, 96], replicated, may hold values from -0.25 to 0.25
- baseline_field: float32 [96, 4096], P(None, 'mesh'), may hold values from -6 to 6
- truth_field: float32 [96, 4096], P(None, 'mesh'), may hold values from -6 to 6
- cell_surface_share: float32 [4096], P('mesh'), may hold values from 0.3 to 3
- node_order: int32 [8, 512], P('mesh'), may hold values from 0 to 511, each once within a row
- query: bfloat16 [8, 4096, 512], P('member', 'mesh'), may hold values from -6 to 6
- key_rows: bfloat16 [8, 4096, 512], P('member', 'mesh'), may hold values from -6 to 6
- value_rows: bfloat16 [8, 4096, 512], P('member', 'mesh'), may hold values from -6 to 6
- row_lse: float32 [8, 8, 4096], P('member', None, 'mesh'), may hold values from 6.5 to 8.5
- kv_owner: int32 [8, 8], replicated, may hold values from 0 to 7, each once within a row
- kv_local: int32 [8, 8], replicated, may hold values from 0 to 3
Outputs:
- grad_query: float32 [8, 4096, 512], P('member', 'mesh')
- grad_key: float32 [8, 4096, 512], P('member', 'mesh')
- grad_value: float32 [8, 4096, 512], P('member', 'mesh')
The draws below stay inside these ranges and needn't reach their ends.
Inputs may be any that keep to these rules, and one draw needn't show every extreme that they name: `kv_owner`: each row names every shard once. `node_order`: each row holds every number of 0 to 511 once.
All inputs are finite; a program needn't handle non-finite values.
Results may differ from the reference program's by a relative error of at most 0.0068.
Values may be sent and summed in bfloat16 or wider, within the bound.
A program may use at most 128 MiB of HBM per device.

```python
import math
import jax
import jax.numpy as jnp
import numpy as np
from jax import lax

CH = 96
HEADS = 8
NODE_DEV = 512
KB = 128
KNB = 8
WIDTH = 512
KBLK_DEV = 4
SHARDS = 8
NODES = 4096
MEMBERS = 8


def with_ends(array, key, low, top_value):
    place = [jax.random.randint(jax.random.fold_in(key, axis), (), 0, length) for axis, length in enumerate(array.shape)]
    longest = array.shape.index(max(array.shape))
    neighbour = place[:longest] + [(place[longest] + 1) % array.shape[longest]] + place[longest + 1:]
    return array.at[tuple(place)].set(low).at[tuple(neighbour)].set(top_value)


def shard_levels(own_key, dims, split, least, high):
    level, own = 1.0, jax.random.fold_in(own_key, 6)
    for axis_at, parts in split:
        heights = jnp.exp(jax.random.uniform(jax.random.fold_in(own, axis_at), (parts,), jnp.float32, least / len(split), high / len(split)))
        level = level * jnp.repeat(heights, dims[axis_at] // parts).reshape([-1 if axis == axis_at else 1 for axis in range(len(dims))])
    return level


def cumulative_ranks(number_of, slope):
    weights = [(1 << 20) // math.isqrt(grade ** slope) + 1 for grade in range(1, number_of + 1)]
    deviation = 1 + sum(weights) // (1 << 30)
    return np.cumsum(np.array([max(1, weight // deviation) for weight in weights]))


def ranked_ids(rng, extent, count, lean):
    listing = cumulative_ranks(count, lean)
    ticket = jax.random.randint(jax.random.fold_in(rng, 1), extent, 0, int(listing[count - 1]))
    grade = jnp.searchsorted(jnp.asarray(listing, jnp.int32), ticket, side="right")
    return jax.random.permutation(jax.random.fold_in(rng, 2), count)[grade].astype(jnp.int32)


def noise(key, shape, width, bound, shards=(), kind=jnp.bfloat16):
    factor_of = shard_levels(key, shape, shards, -0.22, 0.18) if shards else 1.0
    values = jax.random.normal(key, shape, jnp.float32) * width * factor_of
    return jnp.minimum(jnp.maximum(values, -bound), bound).astype(kind)


def setup_inputs(seed: int = 0) -> dict:
    streams_of = jax.random.split(jax.random.key(seed), 13)
    hidden_embedding = noise(streams_of[0], (MEMBERS, NODES, WIDTH), 1.0, 6.0, ((0, 4), (1, 8)))
    decoder_matrix = noise(streams_of[1], (WIDTH, CH), WIDTH ** -0.5, 0.25)
    baseline_field = noise(streams_of[2], (CH, NODES), 1.0, 6.0, ((1, 8),), jnp.float32)
    truth_field = noise(streams_of[3], (CH, NODES), 1.0, 6.0, ((1, 8),), jnp.float32)
    cell_surface_share = jnp.clip(jnp.exp(math.log(3.0) - 2.3025851 * jax.random.uniform(streams_of[4], (NODES,), jnp.float32) ** shard_levels(streams_of[4], (NODES,), ((0, 8),), -0.2, 0.2)), 0.3, 3.0)
    node_order = jax.vmap(lambda own: jax.random.permutation(own, NODE_DEV))(jax.random.split(streams_of[5], SHARDS)).reshape((SHARDS, NODE_DEV)).astype(jnp.int32)
    query = noise(streams_of[6], (MEMBERS, NODES, WIDTH), 1.0, 6.0, ((0, 4), (1, 8)))
    key_rows = noise(streams_of[7], (MEMBERS, NODES, WIDTH), 1.0, 6.0, ((0, 4), (1, 8)))
    value_rows = noise(streams_of[8], (MEMBERS, NODES, WIDTH), 1.0, 6.0, ((0, 4), (1, 8)))
    row_lse = jnp.clip(6.5 + 2.0 * jax.random.uniform(streams_of[9], (MEMBERS, HEADS, NODES), jnp.float32) ** shard_levels(streams_of[9], (MEMBERS, HEADS, NODES), ((0, 4), (2, 8)), -0.2, 0.2), 6.5, 8.5)
    kv_owner = jax.vmap(lambda own: jax.random.permutation(own, SHARDS))(jax.random.split(streams_of[10], SHARDS)).reshape((SHARDS, KNB)).astype(jnp.int32)
    kv_local = with_ends(ranked_ids(streams_of[11], (SHARDS, KNB), KBLK_DEV, 2), jax.random.fold_in(streams_of[11], 3), 0, KBLK_DEV - 1).astype(jnp.int32)
    return {"hidden_embedding": hidden_embedding, "decoder_matrix": decoder_matrix, "baseline_field": baseline_field, "truth_field": truth_field, "cell_surface_share": cell_surface_share, "node_order": node_order, "query": query, "key_rows": key_rows, "value_rows": value_rows, "row_lse": row_lse, "kv_owner": kv_owner, "kv_local": kv_local}


LOSS_SCALE = 4096.0
FAIR_EPS = 0.05
NORM_EPS = 1e-06

def unit_scaled_lines(differences):
    return differences / jnp.sqrt(lax.optimization_barrier(jnp.sum(differences * differences, axis=-2, keepdims=True)) + NORM_EPS)

def outlook_derivative(realization_outlook, truth_field, cell_surface_share):
    realization_list = realization_outlook.shape[0]
    polarity_unit = unit_scaled_lines(realization_outlook - truth_field[None])

    def lone_realization(shard_lines):
        return lax.optimization_barrier(jnp.sum(unit_scaled_lines(shard_lines[None] - realization_outlook), axis=0))
    couple_total = lax.map(lone_realization, realization_outlook)
    weight = LOSS_SCALE * cell_surface_share[None, None, :]
    return weight * (polarity_unit / realization_list - (1.0 - FAIR_EPS) / (realization_list * (realization_list - 1)) * couple_total)

def quantized_entries(numbers):
    return lax.optimization_barrier(numbers.astype(jnp.bfloat16)).astype(jnp.float32)

def tile_grads(queries, grad_rows, log_sums, row_delta, key_tile, value_tile, score_scale):
    scores = jnp.einsum('rhd,khd->hrk', queries, key_tile) * score_scale
    probability = jnp.exp(scores - log_sums[:, :, None])
    dprobs = jnp.einsum('rhd,khd->hrk', grad_rows, value_tile)
    dscores = quantized_entries(probability * (dprobs - row_delta[:, :, None]))
    query_grad = (score_scale * jnp.einsum('hrk,khd->rhd', dscores, key_tile)).astype(jnp.bfloat16)
    key_grad = (score_scale * jnp.einsum('hrk,rhd->khd', dscores, queries)).astype(jnp.bfloat16)
    value_grad = jnp.einsum('hrk,rhd->khd', quantized_entries(probability), grad_rows).astype(jnp.bfloat16)
    return (query_grad, key_grad, value_grad)

def member_grads(arrays, kv_owner, kv_local):
    query, key_rows, value_rows, grad_output, saved_output, row_lse = arrays
    head_count = row_lse.shape[0]
    model_width = query.shape[1]
    head_dim = model_width // head_count
    score_scale = head_dim ** (-0.5)
    split_shape = (SHARDS, NODE_DEV, head_count, head_dim)
    query_blocks = query.astype(jnp.float32).reshape(split_shape)
    grad_blocks = grad_output.astype(jnp.float32).reshape(split_shape)
    saved_blocks = saved_output.astype(jnp.float32).reshape(split_shape)
    row_delta = lax.optimization_barrier(jnp.sum(grad_blocks * saved_blocks, axis=-1)).transpose(0, 2, 1)
    lse_blocks = row_lse.reshape(head_count, SHARDS, NODE_DEV).transpose(1, 0, 2)
    key_blocks = key_rows.astype(jnp.float32).reshape(SHARDS * KBLK_DEV, KB, head_count, head_dim)
    value_blocks = value_rows.astype(jnp.float32).reshape(SHARDS * KBLK_DEV, KB, head_count, head_dim)
    block_ids = (kv_owner * KBLK_DEV + kv_local).astype(jnp.int32)
    zero_grads = jnp.zeros(key_blocks.shape, jnp.float32)

    def per_shard(grads_carry, inputs):
        queries, grad_rows, log_sums, deltas, indices = inputs

        def per_block(running, block_id):
            query_sum, key_grads, value_grads = running
            query_grad, key_grad, value_grad = tile_grads(queries, grad_rows, log_sums, deltas, key_blocks[block_id], value_blocks[block_id], score_scale)
            key_grads = key_grads.at[block_id].add(key_grad.astype(jnp.float32))
            value_grads = value_grads.at[block_id].add(value_grad.astype(jnp.float32))
            return ((query_sum + query_grad.astype(jnp.float32), key_grads, value_grads), None)
        initial = (jnp.zeros(queries.shape, jnp.float32), grads_carry[0], grads_carry[1])
        (query_sum, key_grads, value_grads), unused = lax.scan(per_block, initial, indices)
        return ((key_grads, value_grads), query_sum)
    (key_grads, value_grads), query_sums = lax.scan(per_shard, (zero_grads, zero_grads), (query_blocks, grad_blocks, lse_blocks, row_delta, block_ids))
    return (query_sums.reshape(NODES, model_width), key_grads.reshape(NODES, model_width), value_grads.reshape(NODES, model_width))

def reference(hidden_embedding, decoder_matrix, baseline_field, truth_field, cell_surface_share, node_order, query, key_rows, value_rows, row_lse, kv_owner, kv_local):
    full_coefficient = decoder_matrix.astype(jnp.float32)
    realization_outlook = baseline_field[None] + jnp.einsum('mou,ut->mto', hidden_embedding.astype(jnp.float32), full_coefficient)
    estimate_derivative = quantized_entries(outlook_derivative(realization_outlook, truth_field, cell_surface_share))
    latent_gradient = jnp.einsum('jof,io->jfi', estimate_derivative, full_coefficient).astype(jnp.bfloat16)
    node_index = (node_order + NODE_DEV * jnp.arange(SHARDS, dtype=jnp.int32)[:, None]).reshape(-1).astype(jnp.int32)
    grad_output = jnp.take(latent_gradient, node_index, axis=1)
    saved_output = jnp.take(hidden_embedding, node_index, axis=1)

    def run_member(arrays):
        return member_grads(arrays, kv_owner, kv_local)
    query_grads, key_grads, value_grads = lax.map(run_member, (query, key_rows, value_rows, grad_output, saved_output, row_lse))
    return (query_grads, key_grads, value_grads)
```

```python
import functools

import jax
import jax.numpy as jnp
from jax import lax
from jax.experimental import pallas as pl
from jax.experimental.pallas import tpu as pltpu
from jax.sharding import PartitionSpec as P

KB = 128
LOSS_SCALE = 4096.0
FAIR_EPS = 0.05
NORM_EPS = 1e-06
MESH = pl.DeviceIdType.MESH

NN = (((1,), (0,)), ((), ()))
NT = (((1,), (1,)), ((), ()))
TN = (((0,), (0,)), ((), ()))


def dot(a, b, dims):
    return lax.dot_general(a, b, dims, preferred_element_type=jnp.float32)


def unit(d):
    return d * lax.rsqrt(jnp.sum(d * d, axis=0, keepdims=True) + NORM_EPS)


def listed_block(me, owner_ref, local_ref, s):
    found = jnp.int32(0)
    for j in range(owner_ref.shape[1]):
        found = jnp.where(owner_ref[s, j] == me, local_ref[s, j], found)
    return found


def columns_of(n):
    cols = 1
    while (2 * cols) ** 2 <= n and n % (2 * cols) == 0:
        cols *= 2
    return cols


def fused_kernel(
    groups,
    C,
    R,
    heads,
    owner_ref,
    local_ref,
    hid_in,
    dec_in,
    dect_in,
    base_in,
    truth_in,
    share_in,
    order_in,
    q_in,
    k_in,
    v_in,
    lse_in,
    contrib,
    own_dq,
    hid,
    dec,
    dect,
    base,
    truth,
    share,
    order,
    lse,
    k_vm,
    v_vm,
    fc,
    select,
    saved,
    deriv,
    cols,
    terms,
    q_buf,
    pick_buf,
    kv_buf,
    kvg,
    dqs,
    dqr,
    dq_in,
    grads,
    total,
    ld_sem,
    f_snd,
    f_rcv,
    q_snd,
    q_rcv,
    c_snd,
    c_rcv,
    kv_snd,
    kv_rcv,
    g_snd,
    g_rcv,
    d_snd,
    d_rcv,
):
    D = R // 2
    E = R - 1 - D
    n = R * C
    members, _, rows, width = q_buf.shape
    chans = base.shape[0]
    dim = width // heads
    pair = 2 * dim
    scale = dim ** (-0.5)
    kb = KB
    me = lax.axis_index("mesh")
    grp = lax.axis_index("member")
    r = lax.div(me, C)
    c = lax.rem(me, C)

    def dev(row, col):
        return {"mesh": row * C + col}

    def remote(src, dst, snd, rcv, device):
        return pltpu.make_async_remote_copy(
            src_ref=src, dst_ref=dst, send_sem=snd, recv_sem=rcv, device_id=device, device_id_type=MESH
        )

    loads = [
        (k_in, k_vm),
        (v_in, v_vm),
        (q_in, None),
        (hid_in, hid),
        (dect_in, dect),
        (base_in, base),
        (dec_in, dec),
        (order_in, order),
        (truth_in, truth),
        (share_in, share),
        (lse_in, lse),
    ]

    def load(i):
        src, dst = loads[i]
        if dst is None:
            dst = q_buf.at[:, r]
        return pltpu.make_async_copy(src, dst, ld_sem.at[i])

    for i in (2, 0, 1, 3, 4, 5, 6, 7, 8, 9, 10):
        load(i).start()

    barrier = pltpu.get_barrier_semaphore()
    reach = max(1, E)
    count = jnp.int32(groups - 1)
    for k in range(1, groups):
        pl.semaphore_signal(
            barrier, inc=1, device_id={"member": lax.rem(grp + k, groups)}, device_id_type=MESH
        )
    for off in range(-reach, reach + 1):
        row = r + off
        ok = (row >= 0) & (row < R)
        for k in range(C):
            if off == 0 and k == 0:
                continue
            col = lax.rem(c + k, C)

            @pl.when(ok)
            def _():
                pl.semaphore_signal(barrier, inc=1, device_id=dev(row, col), device_id_type=MESH)

            count = count + jnp.where(ok, 1, 0)
    pl.semaphore_wait(barrier, count)

    def q_copy(m, q, up):
        return remote(
            q_buf.at[m, q],
            q_buf.at[m, q],
            q_snd.at[m, up, q],
            q_rcv.at[m, q],
            dev(r + (1 if up else -1), c),
        )

    def c_copy(q, up, part):
        ref = (cols, terms)[part]
        return remote(
            ref.at[q], ref.at[q], c_snd.at[part, up, q], c_rcv.at[part, q], dev(r + (1 if up else -1), c)
        )

    def passes(up, h):
        if up:
            return r - h, (r - h >= 0) & (r + 1 < R)
        return r + h, (r + h < R) & (r - 1 >= 0)

    def send_q(m, h):
        for up in (1, 0):
            q, ok = passes(up, h)

            @pl.when(ok)
            def _():
                if h > 0:
                    q_copy(m, q, up).wait_recv()
                q_copy(m, q, up).start()

    def send_c(h):
        for up in (1, 0):
            q, ok = passes(up, h)

            @pl.when(ok)
            def _():
                for part in range(2):
                    if h > 0:
                        c_copy(q, up, part).wait_recv()
                    c_copy(q, up, part).start()

    def host_of(s):
        q = lax.div(s, C)
        col = lax.rem(s, C)
        far = jnp.abs(q - r) > D
        row = jnp.where(far, jnp.where(q > r, q - D, q + D), r)
        slot = jnp.where(far, R * C + (jnp.abs(row - r) - 1) * C + c, q * C + c)
        return row, col, slot, (row == r) & (col == c)

    def kv_copy(m, s):
        row, col, slot, _ = host_of(s)
        return remote(
            pick_buf.at[m, s], kv_buf.at[m, slot], kv_snd.at[m, s], kv_rcv.at[m, slot], dev(row, col)
        )

    load(2).wait()
    send_q(0, 0)
    load(0).wait()
    load(1).wait()

    def pick(i, carry):
        m = lax.div(i, n)
        s = lax.rem(i, n)
        block = listed_block(me, owner_ref, local_ref, s)
        _, _, slot, mine = host_of(s)
        key = k_vm[m, block]
        value = v_vm[m, block]

        @pl.when(mine)
        def _():
            kv_buf[m, slot, 0] = key
            kv_buf[m, slot, 1] = value

        @pl.when(jnp.logical_not(mine))
        def _():
            pick_buf[m, s, 0] = key
            pick_buf[m, s, 1] = value

        return carry

    lax.fori_loop(0, members * n, pick, 0)

    def send_kv(i, carry):
        m = lax.div(i, n)
        s = lax.rem(i, n)

        @pl.when(jnp.logical_not(host_of(s)[3]))
        def _():
            kv_copy(m, s).start()

        return carry

    for i in (3, 4, 5):
        load(i).wait()
    for m in range(members):
        fc[grp, m] = base[...] + dot(dect[...], hid[m], NT)
    lax.fori_loop(0, members * n, send_kv, 0)
    mate = grp + 1 - 2 * lax.rem(grp, 2)

    def f_copy(src, sem, to):
        return remote(fc.at[src], fc.at[src], f_snd.at[sem], f_rcv.at[src], {"member": to})

    cousins = range(1, groups // 2)
    for k in cousins:
        f_copy(grp, k, lax.rem(grp + 2 * k, groups)).start()
    f_copy(grp, 0, mate).start()

    for i in range(6, 11):
        load(i).wait()
    select[...] = (
        lax.broadcasted_iota(jnp.int32, (rows, rows), 0) == order[...]
    ).astype(jnp.bfloat16)
    for m in range(members):
        saved[m] = dot(hid[m], select[...], TN).astype(jnp.bfloat16)
        terms[r, m, pl.ds(0, heads)] = lse[m]

    for h in range(1, D):
        send_q(0, h)
    for k in cousins:
        src = lax.rem(grp + 2 * k, groups)
        f_copy(src, 0, mate).wait_recv()
        f_copy(src, groups // 2 + k, mate).start()
    for k in range(groups // 2):
        f_copy(lax.rem(mate + 2 * k, groups), 0, mate).wait_recv()

    everyone = members * groups
    lanes_step = 128

    def score(i, carry):
        lanes = pl.ds(pl.multiple_of(i * lanes_step, lanes_step), lanes_step)
        weight = LOSS_SCALE * share[:, lanes]
        for m in range(members):
            own = fc[grp, m, :, lanes]
            couple = jnp.zeros_like(own)
            for other in range(groups):
                for k in range(members):
                    couple = couple + unit(own - fc[other, k, :, lanes])
            polarity = unit(own - truth[:, lanes])
            deriv[m, :, lanes] = (
                weight
                * (polarity / everyone - (1.0 - FAIR_EPS) / (everyone * (everyone - 1)) * couple)
            ).astype(jnp.bfloat16)
        return carry

    lax.fori_loop(0, rows // lanes_step, score, 0)

    def latent(m, column):
        grads[...] = dot(dec[...], column, NN).astype(jnp.bfloat16)

    for m in range(members):
        column = dot(deriv[m], select[...], NN).astype(jnp.bfloat16)
        cols[r, m] = column
        latent(m, column)
        for h in range(heads):
            part = pl.ds(h * dim, dim)
            terms[r, m, pl.ds(heads + h, 1)] = jnp.sum(
                grads[part].astype(jnp.float32) * saved[m, part].astype(jnp.float32),
                axis=0,
                keepdims=True,
            )
    send_c(0)
    for m in range(1, members):
        send_q(m, 0)
    for h in range(1, D):
        send_c(h)

    low = lax.broadcasted_iota(jnp.int32, (kb, pair), 1) < dim

    def tile(m, q, slot):
        for p in range(heads // 2):
            lanes = pl.ds(p * pair, pair)
            key = kv_buf[m, slot, 0, :, lanes]
            value = kv_buf[m, slot, 1, :, lanes]
            nought = jnp.zeros_like(key)
            keys = jnp.concatenate(
                [jnp.where(low, key, nought), jnp.where(low, nought, key)], axis=0
            )
            values = jnp.concatenate(
                [jnp.where(low, value, nought), jnp.where(low, nought, value)], axis=0
            )
            q_pair = q_buf[m, q, :, lanes]
            g_pair = grads[lanes, :]
            scores = dot(keys, q_pair, NT)
            dprobs = dot(values, g_pair, NN)
            prob, dscore = [], []
            for k in range(2):
                part = slice(k * kb, (k + 1) * kb)
                h = 2 * p + k
                pr = jnp.exp(scores[part] * scale - terms[q, m, pl.ds(h, 1), :])
                prob.append(pr.astype(jnp.bfloat16))
                dscore.append(
                    (pr * (dprobs[part] - terms[q, m, pl.ds(heads + h, 1), :])).astype(jnp.bfloat16)
                )
            prob = jnp.concatenate(prob, axis=0)
            dscore = jnp.concatenate(dscore, axis=0)
            dv = dot(prob, g_pair, NT)
            dk = dot(dscore, q_pair, NN) * scale
            kvg[m, slot, 0, :, lanes] = jnp.where(low, dk[:kb], dk[kb:]).astype(jnp.bfloat16)
            kvg[m, slot, 1, :, lanes] = jnp.where(low, dv[:kb], dv[kb:]).astype(jnp.bfloat16)
            total[lanes, :] += dot(keys, dscore, TN)

    def tile_place(q, t):
        below = q > r
        turn = lax.div(t, C)
        row = jnp.where(below, r - turn, r + turn)
        slot = jnp.where(turn == 0, q * C + t, R * C + t - C)
        return row, lax.rem(t, C), slot, t == c

    def tile_count(q):
        extra = jnp.where(q == r + D, r, jnp.where(q == r - D, R - 1 - r, 0))
        return C * (1 + extra)

    def g_copy(m, q, t):
        row, col, slot, _ = tile_place(q, t)
        return remote(
            kvg.at[m, slot],
            contrib.at[m, q * C + c],
            g_snd.at[m, slot],
            g_rcv.at[m, q * C + c],
            dev(row, col),
        )

    def g_local(m, q, t):
        _, _, slot, _ = tile_place(q, t)
        return pltpu.make_async_copy(
            kvg.at[m, slot], contrib.at[m, q * C + c], g_rcv.at[m, q * C + c]
        )

    def kv_arrival(m, slot):
        return remote(
            pick_buf.at[0, 0], kv_buf.at[m, slot], kv_snd.at[0, 0], kv_rcv.at[m, slot], dev(r, c)
        )

    def d_copy(m, q, up, last):
        if last:
            dst, sem = dq_in.at[m, 1 - up], d_rcv.at[m, R + 1 - up]
        else:
            dst, sem = dqr.at[m, q], d_rcv.at[m, q]
        return remote(dqs.at[m, q], dst, d_snd.at[m, q], sem, dev(r + (1 if up else -1), c))

    def order_of(step):
        dist = D - lax.div(step, 2)
        q = jnp.where(lax.rem(step, 2) == 0, r + dist, r - dist)
        return q, dist, (q >= 0) & (q < R)

    def job(i, carry):
        m = lax.div(i, 2 * D + 1)
        step = lax.rem(i, 2 * D + 1)
        q, dist, ok = order_of(step)

        @pl.when((step == 2 * D) & (m + 1 < members))
        def _():
            for h in range(1, D):
                send_q(m + 1, h)

        @pl.when(ok)
        def _():
            for up in (1, 0):
                edge = (r == R - 1) if up else (r == 0)
                here = ((q < r) if up else (q > r)) & ((dist == D) | edge)

                @pl.when(here)
                def _():
                    q_copy(m, q, up).wait_recv()

                    @pl.when(m == 0)
                    def _():
                        c_copy(q, up, 0).wait_recv()
                        c_copy(q, up, 1).wait_recv()

            latent(m, cols[q, m])
            total[...] = jnp.zeros_like(total)

            def one(t, carry):
                _, _, slot, mine = tile_place(q, t)

                @pl.when(jnp.logical_not(mine))
                def _():
                    kv_arrival(m, slot).wait_recv()

                tile(m, q, slot)

                @pl.when(mine)
                def _():
                    g_local(m, q, t).start()

                @pl.when(jnp.logical_not(mine))
                def _():
                    g_copy(m, q, t).start()

                return carry

            lax.fori_loop(0, tile_count(q), one, 0)

            @pl.when(dist == 0)
            def _():
                own_dq[m] = total[...] * scale

            for up in (1, 0):
                side = (q > r) if up else (q < r)
                chained = (dist < D) & ((r > 0) if up else (r < R - 1))

                @pl.when(side & chained)
                def _():
                    d_copy(m, q, up, False).wait_recv()
                    dqs[m, q] = (total[...] * scale + dqr[m, q].astype(jnp.float32)).astype(
                        jnp.bfloat16
                    )

                @pl.when(side & jnp.logical_not(chained))
                def _():
                    dqs[m, q] = (total[...] * scale).astype(jnp.bfloat16)

                @pl.when(side & (dist == 1))
                def _():
                    d_copy(m, q, up, True).start()

                @pl.when(side & (dist > 1))
                def _():
                    d_copy(m, q, up, False).start()

        return carry

    lax.fori_loop(0, members * (2 * D + 1), job, 0)

    for m in range(members):
        for up in (1, 0):
            @pl.when((r > 0) if up else (r < R - 1))
            def _():
                d_copy(m, r, up, True).wait_recv()
                own_dq[m] = own_dq[m] + dq_in[m, 1 - up].astype(jnp.float32)

    def last(i, carry):
        m = lax.div(i, n)
        s = lax.rem(i, n)
        pltpu.make_async_copy(kvg.at[0, 0], contrib.at[m, s], g_rcv.at[m, s]).wait()

        @pl.when(jnp.logical_not(host_of(s)[3]))
        def _():
            kv_copy(m, s).wait_send()

        return carry

    lax.fori_loop(0, members * n, last, 0)

    def sent(i, carry):
        m = lax.div(i, 2 * D + 1)
        q, dist, ok = order_of(lax.rem(i, 2 * D + 1))

        @pl.when(ok)
        def _():
            def one(t, carry):
                @pl.when(jnp.logical_not(tile_place(q, t)[3]))
                def _():
                    g_copy(m, q, t).wait_send()

                return carry

            lax.fori_loop(0, tile_count(q), one, 0)

            @pl.when(dist > 0)
            def _():
                d_copy(m, q, 1, False).wait_send()

        return carry

    lax.fori_loop(0, members * (2 * D + 1), sent, 0)
    for h in range(D):
        for up in (1, 0):
            q, ok = passes(up, h)

            @pl.when(ok)
            def _():
                for m in range(members):
                    q_copy(m, q, up).wait_send()
                for part in range(2):
                    c_copy(q, up, part).wait_send()

    f_copy(grp, 0, mate).wait_send()
    for k in cousins:
        f_copy(grp, k, mate).wait_send()
        f_copy(grp, groups // 2 + k, mate).wait_send()


def fused(groups, n, heads, blocks, arrays):
    (_, _, hid, dec, dect, base, truth, share, order, q, k, v, lse) = arrays
    C = columns_of(n)
    R = n // C
    D = R // 2
    E = R - 1 - D
    members, rows, width = hid.shape
    chans = base.shape[0]
    bf, f32 = jnp.bfloat16, jnp.float32
    slots = (R + E) * C
    vm = pltpu.VMEM
    dma = pltpu.SemaphoreType.DMA
    scratch = [
        vm(hid.shape, bf),
        vm(dec.shape, bf),
        vm(dect.shape, bf),
        vm(base.shape, f32),
        vm(truth.shape, f32),
        vm(share.shape, f32),
        vm(order.shape, jnp.int32),
        vm(lse.shape, f32),
        vm(k.shape, bf),
        vm(v.shape, bf),
        vm((groups, members, chans, rows), f32),
        vm((rows, rows), bf),
        vm((members, width, rows), bf),
        vm((members, chans, rows), bf),
        vm((R, members, chans, rows), bf),
        vm((R, members, 2 * heads, rows), f32),
        vm((members, R, rows, width), bf),
        vm((members, n, 2, KB, width), bf),
        vm((members, slots, 2, KB, width), bf),
        vm((members, slots, 2, KB, width), bf),
        vm((members, R, width, rows), bf),
        vm((members, R, width, rows), bf),
        vm((members, 2, width, rows), bf),
        vm((width, rows), bf),
        vm((width, rows), f32),
        dma((11,)),
        dma((groups,)),
        dma((groups,)),
        dma((members, 2, R)),
        dma((members, R)),
        dma((2, 2, R)),
        dma((2, R)),
        dma((members, n)),
        dma((members, slots)),
        dma((members, slots)),
        dma((members, n)),
        dma((members, R)),
        dma((members, R + 2)),
    ]
    smem = pl.BlockSpec(memory_space=pltpu.SMEM)
    anyw = pl.BlockSpec(memory_space=pl.ANY)
    tiles = members * n
    return pl.pallas_call(
        functools.partial(fused_kernel, groups, C, R, heads),
        out_shape=[
            jax.ShapeDtypeStruct((members, n, 2, KB, width), bf),
            jax.ShapeDtypeStruct((members, width, rows), f32),
        ],
        in_specs=[smem, smem] + [anyw] * 11,
        out_specs=[anyw, pl.BlockSpec(memory_space=pltpu.VMEM)],
        scratch_shapes=scratch,
        compiler_params=pltpu.CompilerParams(
            collective_id=0, has_side_effects=True, vmem_limit_bytes=60 * 2**20
        ),
        cost_estimate=pl.CostEstimate(
            flops=tiles * 10 * rows * KB * width,
            bytes_accessed=16 * 2**20,
            transcendentals=tiles * heads * rows * KB,
        ),
        name="fused",
    )(*arrays)


def collect_kernel(me_ref, owner_ref, local_ref, contrib, own_dq, gq, gk, gv):
    gq[0] = own_dq[0].T
    gk[...] = jnp.zeros_like(gk)
    gv[...] = jnp.zeros_like(gv)
    for s in range(contrib.shape[1]):
        block = listed_block(me_ref[0], owner_ref, local_ref, s)
        gk[0, block] += contrib[0, s, 0].astype(jnp.float32)
        gv[0, block] += contrib[0, s, 1].astype(jnp.float32)


def collect(blocks, tables, contrib, own_dq):
    members, n, _, kb, width = contrib.shape
    rows = own_dq.shape[2]
    steps = 4
    kv_shape = jax.ShapeDtypeStruct((members, blocks, kb, width), jnp.float32)
    kv_spec = pl.BlockSpec((1, blocks, kb // steps, width), lambda m, i, *_: (m, 0, i, 0))
    return pl.pallas_call(
        collect_kernel,
        out_shape=[jax.ShapeDtypeStruct((members, rows, width), jnp.float32), kv_shape, kv_shape],
        grid_spec=pltpu.PrefetchScalarGridSpec(
            num_scalar_prefetch=3,
            grid=(members, steps),
            in_specs=[
                pl.BlockSpec((1, n, 2, kb // steps, width), lambda m, i, *_: (m, 0, 0, i, 0)),
                pl.BlockSpec((1, width, rows // steps), lambda m, i, *_: (m, 0, i)),
            ],
            out_specs=[
                pl.BlockSpec((1, rows // steps, width), lambda m, i, *_: (m, i, 0)),
                kv_spec,
                kv_spec,
            ],
        ),
        compiler_params=pltpu.CompilerParams(vmem_limit_bytes=24 * 2**20),
        cost_estimate=pl.CostEstimate(flops=10**6, bytes_accessed=12 * 2**20, transcendentals=0),
        name="collect",
    )(*tables, contrib, own_dq)


def shards(
    groups,
    n,
    hidden_embedding,
    decoder_matrix,
    baseline_field,
    truth_field,
    cell_surface_share,
    node_order,
    query,
    key_rows,
    value_rows,
    row_lse,
    kv_owner,
    kv_local,
):
    members, nodes, width = hidden_embedding.shape
    heads = row_lse.shape[1]
    blocks = nodes // KB
    split = (members, blocks, KB, width)
    contrib, own_dq = fused(
        groups,
        n,
        heads,
        blocks,
        (
            kv_owner,
            kv_local,
            hidden_embedding,
            decoder_matrix,
            decoder_matrix.T,
            baseline_field,
            truth_field,
            cell_surface_share[None],
            node_order,
            query,
            key_rows.reshape(split),
            value_rows.reshape(split),
            row_lse,
        ),
    )
    me = jnp.full((1,), lax.axis_index("mesh"), jnp.int32)
    gq, gk, gv = collect(blocks, (me, kv_owner, kv_local), contrib, own_dq)
    return gq, gk.reshape(key_rows.shape), gv.reshape(value_rows.shape)


def solution(mesh):
    rows = P("member", "mesh", None)
    return jax.shard_map(
        functools.partial(shards, mesh.shape["member"], mesh.shape["mesh"]),
        mesh=mesh,
        in_specs=(
            rows,
            P(),
            P(None, "mesh"),
            P(None, "mesh"),
            P("mesh"),
            P("mesh", None),
            rows,
            rows,
            rows,
            P("member", None, "mesh"),
            P(),
            P(),
        ),
        out_specs=(rows, rows, rows),
        check_vma=False,
    )
```

```python
import functools
import math

import jax
import jax.numpy as jnp
from jax import lax
from jax.experimental import pallas as pl
from jax.experimental.pallas import tpu as pltpu
from jax.sharding import PartitionSpec as P

KB = 128
LOSS_SCALE = 4096.0
FAIR_EPS = 0.05
NORM_EPS = 1e-06
PIECES = 2
VMEM_LIMIT = 63 * 2**20
VMEM_SPARE = 2 * 2**20
VMEM_GAP = 2**19
MESH = pl.DeviceIdType.MESH

NN = (((1,), (0,)), ((), ()))
NT = (((1,), (1,)), ((), ()))
TN = (((0,), (0,)), ((), ()))


def dot(a, b, dims):
    return lax.dot_general(a, b, dims, preferred_element_type=jnp.float32)


def unit(d):
    return d * lax.rsqrt(jnp.sum(d * d, axis=0, keepdims=True) + NORM_EPS)


def listed_block(me, owner_ref, local_ref, s):
    found = jnp.int32(0)
    for j in range(owner_ref.shape[1]):
        found = jnp.where(owner_ref[s, j] == me, local_ref[s, j], found)
    return found


def columns_of(n):
    cols = 1
    while (2 * cols) ** 2 <= n and n % (2 * cols) == 0:
        cols *= 2
    return cols


def fused_kernel(
    groups,
    C,
    R,
    heads,
    near,
    owner_ref,
    local_ref,
    hid_in,
    dect_in,
    base_in,
    truth_in,
    share_in,
    order_in,
    q_in,
    k_in,
    v_in,
    lse_in,
    gq_out,
    gk_out,
    gv_out,
    land,
    hid,
    dect,
    base,
    truth,
    share,
    order,
    lse,
    k_vm,
    v_vm,
    fc,
    select,
    deriv,
    cols,
    terms,
    q_buf,
    pick_buf,
    kv_buf,
    kvg,
    kv_sum,
    dq_sum,
    acc,
    part,
    dqs,
    dqr,
    dq_in,
    grads,
    total,
    ld_sem,
    f_snd,
    f_rcv,
    q_snd,
    q_rcv,
    c_snd,
    c_rcv,
    kv_snd,
    kv_rcv,
    g_snd,
    g_rcv,
    d_snd,
    d_rcv,
    l_rcv,
    o_sem,
    stage,
):
    D = R // 2
    E = R - 1 - D
    n = R * C
    members, _, rows, width = q_buf.shape
    dim = width // heads
    pair = 2 * dim
    scale = dim ** (-0.5)
    kb = KB
    me = lax.axis_index("mesh")
    grp = lax.axis_index("member")
    r = lax.div(me, C)
    c = lax.rem(me, C)
    mate = grp + 1 - 2 * lax.rem(grp, 2)
    cousins = range(1, groups // 2)

    def dev(row, col):
        return {"mesh": row * C + col}

    def remote(src, dst, snd, rcv, device):
        return pltpu.make_async_remote_copy(
            src_ref=src, dst_ref=dst, send_sem=snd, recv_sem=rcv, device_id=device, device_id_type=MESH
        )

    loads = [
        (q_in, None),
        (hid_in, hid),
        (dect_in, dect),
        (base_in, base),
        (k_in, k_vm),
        (v_in, v_vm),
        (order_in, order),
        (truth_in, truth),
        (share_in, share),
        (lse_in, lse),
    ]

    def load(i):
        src, dst = loads[i]
        if dst is None:
            dst = q_buf.at[:, r]
        return pltpu.make_async_copy(src, dst, ld_sem.at[i])

    barrier = pltpu.get_barrier_semaphore()

    def greet(device):
        pl.semaphore_signal(barrier, inc=1, device_id=device, device_id_type=MESH)

    greet({"member": mate})
    for k in cousins:
        greet({"member": lax.rem(grp + 2 * k, groups)})
    count = jnp.int32(groups // 2)
    reach = max(1, E)
    for off in range(-reach, reach + 1):
        row = r + off
        ok = (row >= 0) & (row < R)
        for k in range(C):
            if off == 0 and k == 0:
                continue
            col = lax.rem(c + k, C)

            @pl.when(ok)
            def _():
                greet(dev(row, col))

            count = count + jnp.where(ok, 1, 0)

    for i in range(len(loads)):
        load(i).start()
    for i in range(1, 4):
        load(i).wait()
    for m in range(members):
        fc[grp, m] = base[...] + dot(dect[...], hid[m], NT)
    load(0).wait()
    pl.semaphore_wait(barrier, count)

    half = rows // PIECES

    def q_copy(m, q, up, piece):
        ref = q_buf.at[m, q, pl.ds(piece * half, half)]
        return remote(
            ref, ref, q_snd.at[m, up, q, piece], q_rcv.at[m, q, piece], dev(r + (1 if up else -1), c)
        )

    def c_copy(q, up, kind):
        ref = (cols, terms)[kind]
        return remote(
            ref.at[q], ref.at[q], c_snd.at[kind, up, q], c_rcv.at[kind, q], dev(r + (1 if up else -1), c)
        )

    def passes(up, h):
        if up:
            return r - h, (r - h >= 0) & (r + 1 < R)
        return r + h, (r + h < R) & (r - 1 >= 0)

    def send_q(m, h, pieces):
        for piece in pieces:
            for up in (1, 0):
                q, ok = passes(up, h)

                @pl.when(ok)
                def _():
                    if h > 0:
                        q_copy(m, q, up, piece).wait_recv()
                    q_copy(m, q, up, piece).start()

    def send_c(h):
        for up in (1, 0):
            q, ok = passes(up, h)

            @pl.when(ok)
            def _():
                for kind in range(2):
                    if h > 0:
                        c_copy(q, up, kind).wait_recv()
                    c_copy(q, up, kind).start()

    def host_of(s):
        q = lax.div(s, C)
        col = lax.rem(s, C)
        far = jnp.abs(q - r) > D
        row = jnp.where(far, jnp.where(q > r, q - D, q + D), r)
        slot = jnp.where(far, R * C + (jnp.abs(row - r) - 1) * C + c, q * C + c)
        return row, col, slot, far

    def kv_copy(m, s):
        row, col, slot, _ = host_of(s)
        return remote(
            pick_buf.at[m, s], kv_buf.at[m, slot], kv_snd.at[m, s], kv_rcv.at[m, slot], dev(row, col)
        )

    def send_near(m):
        def one(i, carry):
            dist = lax.div(i + 1, 2)
            q = jnp.where(lax.rem(i, 2) == 0, r + dist, r - dist)
            ok = (q >= 0) & (q < R)
            for k in range(1, C):

                @pl.when(ok)
                def _():
                    kv_copy(m, q * C + lax.rem(c + k, C)).start()

            return carry

        lax.fori_loop(0, 2 * D + 1, one, 0)

    def send_far(m, straight):
        def one(q, carry):
            @pl.when(jnp.abs(q - r) > D)
            def _():
                for k in range(0, 1) if straight else range(1, C):
                    kv_copy(m, q * C + lax.rem(c + k, C)).start()

            return carry

        if E > 0:
            lax.fori_loop(0, R, one, 0)

    def f_copy(src, sem, to):
        return remote(fc.at[src], fc.at[src], f_snd.at[sem], f_rcv.at[src], {"member": to})

    send_q(0, 0, range(PIECES))
    for k in cousins:
        f_copy(grp, k, lax.rem(grp + 2 * k, groups)).start()
    f_copy(grp, 0, mate).start()
    load(4).wait()
    load(5).wait()

    def pick(i, carry):
        m = lax.div(i, n)
        s = lax.rem(i, n)
        block = listed_block(me, owner_ref, local_ref, s)
        row, col, slot, _ = host_of(s)
        mine = (row == r) & (col == c)
        key = k_vm[m, block]
        value = v_vm[m, block]

        @pl.when(mine)
        def _():
            kv_buf[m, slot, 0] = key
            kv_buf[m, slot, 1] = value

        @pl.when(jnp.logical_not(mine))
        def _():
            pick_buf[m, s, 0] = key
            pick_buf[m, s, 1] = value

        return carry

    lax.fori_loop(0, members * n, pick, 0)
    for i in range(6, len(loads)):
        load(i).wait()
    select[...] = (
        lax.broadcasted_iota(jnp.int32, (rows, rows), 0) == order[...]
    ).astype(jnp.bfloat16)
    send_near(0)
    send_far(0, True)
    for m in range(members):
        dqs[m, 0, 0] = dot(hid[m], select[...], TN).astype(jnp.bfloat16)
        terms[r, m, pl.ds(0, heads)] = lse[m]

    for h in range(1, D):
        send_q(0, h, range(1))
    for k in cousins:
        src = lax.rem(grp + 2 * k, groups)
        f_copy(src, 0, mate).wait_recv()
        f_copy(src, groups // 2 + k, mate).start()
    for k in range(groups // 2):
        f_copy(lax.rem(mate + 2 * k, groups), 0, mate).wait_recv()

    everyone = members * groups
    lanes_step = 128

    def score(i, carry):
        lanes = pl.ds(pl.multiple_of(i * lanes_step, lanes_step), lanes_step)
        weight = LOSS_SCALE * share[:, lanes]
        for m in range(members):
            own = fc[grp, m, :, lanes]
            couple = jnp.zeros_like(own)
            for other in range(groups):
                for k in range(members):
                    couple = couple + unit(own - fc[other, k, :, lanes])
            polarity = unit(own - truth[:, lanes])
            deriv[m, :, lanes] = (
                weight
                * (polarity / everyone - (1.0 - FAIR_EPS) / (everyone * (everyone - 1)) * couple)
            ).astype(jnp.bfloat16)
        return carry

    lax.fori_loop(0, rows // lanes_step, score, 0)

    def latent(column):
        grads[...] = dot(dect[...], column, TN).astype(jnp.bfloat16)

    for m in range(members):
        column = dot(deriv[m], select[...], NN).astype(jnp.bfloat16)
        cols[r, m] = column
        latent(column)
        for h in range(heads):
            span = pl.ds(h * dim, dim)
            terms[r, m, pl.ds(heads + h, 1)] = jnp.sum(
                grads[span].astype(jnp.float32) * dqs[m, 0, 0, span].astype(jnp.float32),
                axis=0,
                keepdims=True,
            )
    send_c(0)
    for h in range(1, D):
        send_q(0, h, range(1, PIECES))
    send_far(0, False)
    for m in range(1, members):
        send_near(m)

    low = lax.broadcasted_iota(jnp.int32, (kb, pair), 1) < dim

    def tile(m, q, slot):
        for p in range(heads // 2):
            lanes = pl.ds(p * pair, pair)
            key = kv_buf[m, slot, 0, :, lanes]
            value = kv_buf[m, slot, 1, :, lanes]
            nought = jnp.zeros_like(key)
            keys = jnp.concatenate(
                [jnp.where(low, key, nought), jnp.where(low, nought, key)], axis=0
            )
            values = jnp.concatenate(
                [jnp.where(low, value, nought), jnp.where(low, nought, value)], axis=0
            )
            q_pair = q_buf[m, q, :, lanes]
            g_pair = grads[lanes, :]
            scores = dot(keys, q_pair, NT)
            dprobs = dot(values, g_pair, NN)
            prob, dscore = [], []
            for k in range(2):
                span = slice(k * kb, (k + 1) * kb)
                h = 2 * p + k
                pr = jnp.exp(scores[span] * scale - terms[q, m, pl.ds(h, 1), :])
                prob.append(pr.astype(jnp.bfloat16))
                dscore.append(
                    (pr * (dprobs[span] - terms[q, m, pl.ds(heads + h, 1), :])).astype(jnp.bfloat16)
                )
            prob = jnp.concatenate(prob, axis=0)
            dscore = jnp.concatenate(dscore, axis=0)
            dv = dot(prob, g_pair, NT)
            dk = dot(dscore, q_pair, NN) * scale
            kvg[m, slot, 0, :, lanes] = jnp.where(low, dk[:kb], dk[kb:]).astype(jnp.bfloat16)
            kvg[m, slot, 1, :, lanes] = jnp.where(low, dv[:kb], dv[kb:]).astype(jnp.bfloat16)
            total[lanes, :] += dot(keys, dscore, TN)

    def tile_place(q, t):
        turn = lax.div(t, C)
        row = jnp.where(q > r, r - turn, r + turn)
        slot = jnp.where(turn == 0, q * C + t, R * C + t - C)
        return row, lax.rem(t, C), slot, t == c

    def tile_count(q):
        extra = jnp.where(q == r + D, r, jnp.where(q == r - D, R - 1 - r, 0))
        return C * (1 + extra)

    def g_copy(m, q, t):
        row, col, slot, _ = tile_place(q, t)
        return remote(
            kvg.at[m, slot],
            land.at[m, q * C + c],
            g_snd.at[m, slot],
            g_rcv.at[m, q * C + c],
            dev(row, col),
        )

    def kv_arrival(m, slot):
        return remote(
            pick_buf.at[0, 0], kv_buf.at[m, slot], kv_snd.at[0, 0], kv_rcv.at[m, slot], dev(r, c)
        )

    def d_copy(m, dist, side, last):
        src, snd = dqs.at[m, dist - 1, side], d_snd.at[m, dist - 1, side]
        device = dev(r + 1 - 2 * side, c)
        if last:
            return remote(src, dq_in.at[m, side], snd, l_rcv.at[m, side], device)
        return remote(src, dqr.at[m, dist - 2, side], snd, d_rcv.at[m, dist - 2, side], device)

    plan = [(0, 0)] + [(0, d) for d in range(1, D)]
    plan += [(m, 0) for m in range(1, members)] + [(0, D)]
    relay_at = len(plan)
    for m in range(1, members):
        plan += [(m, d) for d in range(1, D + 1)]

    def table(step, values):
        found = jnp.int32(values[0])
        for k, value in enumerate(values):
            found = jnp.where(step == k, jnp.int32(value), found)
        return found

    def job(i, carry):
        step = lax.div(i, 2)
        side = lax.rem(i, 2)
        m = table(step, [a for a, _ in plan])
        dist = table(step, [b for _, b in plan])
        q = r + dist - 2 * dist * side
        ok = (q >= 0) & (q < R) & ((dist > 0) | (side == 0))

        @pl.when(i == 2)
        def _():
            for h in range(1, D):
                send_c(h)
            for k in range(1, members):
                send_q(k, 0, range(PIECES))
            for k in range(1, members):
                send_far(k, True)
                send_far(k, False)

        @pl.when(i == 2 * relay_at)
        def _():
            for k in range(1, members):
                for h in range(1, D):
                    send_q(k, h, range(PIECES))
            for far_side in range(2):
                far_q = r + D - 2 * D * far_side

                @pl.when((far_q >= 0) & (far_q < R))
                def _():
                    d_copy(0, D, far_side, D == 1).start()

                    def late(t, carry):
                        g_copy(0, far_q, t).start()
                        return carry

                    lax.fori_loop(C, tile_count(far_q), late, 0)

        @pl.when(ok)
        def _():
            for up in (1, 0):
                edge = (r == R - 1) if up else (r == 0)
                here = ((q < r) if up else (q > r)) & ((dist == D) | edge)

                @pl.when(here)
                def _():
                    for piece in range(PIECES):
                        q_copy(m, q, up, piece).wait_recv()

                    @pl.when(m == 0)
                    def _():
                        c_copy(q, up, 0).wait_recv()
                        c_copy(q, up, 1).wait_recv()

            latent(cols[q, m])
            total[...] = jnp.zeros_like(total)

            def one(t, carry):
                _, _, slot, mine = tile_place(q, t)

                @pl.when(jnp.logical_not(mine))
                def _():
                    kv_arrival(m, slot).wait_recv()

                tile(m, q, slot)

                @pl.when(jnp.logical_not(mine) & ((t < C) | (m > 0)))
                def _():
                    g_copy(m, q, t).start()

                return carry

            lax.fori_loop(0, tile_count(q), one, 0)

            @pl.when(dist == 0)
            def _():
                acc[m] = total[...] * scale

            @pl.when((dist > 0) & (dist < D))
            def _():
                part[m, jnp.minimum(jnp.maximum(dist - 1, 0), max(D - 2, 0)), side] = total[...] * scale

            @pl.when(dist == D)
            def _():
                dqs[m, D - 1, side] = (total[...] * scale).astype(jnp.bfloat16)

                @pl.when(m > 0)
                def _():
                    d_copy(m, D, side, D == 1).start()

        return carry

    lax.fori_loop(0, 2 * len(plan), job, 0)

    for m in range(members):
        for dist in range(D - 1, 0, -1):
            for side in range(2):
                q = r + dist - 2 * dist * side
                chained = (r > 0) if side == 0 else (r < R - 1)
                ok = (q >= 0) & (q < R)

                @pl.when(ok & chained)
                def _():
                    d_copy(m, dist + 1, side, False).wait_recv()
                    dqs[m, dist - 1, side] = (
                        part[m, dist - 1, side] + dqr[m, dist - 1, side].astype(jnp.float32)
                    ).astype(jnp.bfloat16)

                @pl.when(ok & jnp.logical_not(chained))
                def _():
                    dqs[m, dist - 1, side] = part[m, dist - 1, side].astype(jnp.bfloat16)

                @pl.when(ok)
                def _():
                    d_copy(m, dist, side, dist == 1).start()

    def kv_out(m, kind):
        return pltpu.make_async_copy(kv_sum.at[m, kind], (gk_out, gv_out)[kind].at[m], o_sem.at[m, kind])

    def q_out(m):
        return pltpu.make_async_copy(dq_sum.at[m], gq_out.at[m], o_sem.at[m, 2])

    def landed(ref, m, s, col, row):
        return remote(kvg.at[0, 0], ref, g_snd.at[0, 0], g_rcv.at[m, s], dev(row, col))

    chunk = 32

    def gather(m):
        kv_sum[m] = jnp.zeros_like(kv_sum[m])

        def one(i, carry):
            dist = lax.div(i, 2 * C)
            side = lax.rem(lax.div(i, C), 2)
            q = r + dist - 2 * dist * side
            ok = (q >= 0) & (q < R) & ((dist > 0) | (side == 0))

            @pl.when(ok)
            def _():
                s = q * C + lax.rem(i, C)
                row, col, slot, _ = host_of(s)
                mine = (row == r) & (col == c)
                block = listed_block(me, owner_ref, local_ref, s)

                def add(ref, a, b):
                    def rows_of(j, carry):
                        span = pl.ds(pl.multiple_of(j * chunk, chunk), chunk)
                        for kind in range(2):
                            value = ref[a, b, kind, span].astype(jnp.float32)
                            for k in range(kv_sum.shape[2]):
                                kv_sum[m, kind, k, span] += jnp.where(block == k, value, 0.0)
                        return carry

                    lax.fori_loop(0, kb // chunk, rows_of, 0)

                @pl.when(mine)
                def _():
                    add(kvg, m, slot)

                @pl.when(jnp.logical_not(mine))
                def _():
                    landed(land.at[m, s], m, s, col, row).wait_recv()
                    if near:
                        add(land, m, s)
                    else:
                        bring = pltpu.make_async_copy(land.at[m, s], stage.at[0, 0], ld_sem.at[0])
                        bring.start()
                        bring.wait()
                        add(stage, 0, 0)

            return carry

        lax.fori_loop(0, 2 * C * R, one, 0)
        for kind in range(2):
            kv_out(m, kind).start()

    for m in range(members):
        gather(m)
    for m in range(members):
        for side in range(2):
            @pl.when((r > 0) if side == 0 else (r < R - 1))
            def _():
                d_copy(m, 1, side, True).wait_recv()
                acc[m] = acc[m] + dq_in[m, side].astype(jnp.float32)
        dq_sum[m] = acc[m].T
        q_out(m).start()

    def last(i, carry):
        m = lax.div(i, n)
        s = lax.rem(i, n)
        row, col, _, _ = host_of(s)

        @pl.when((row != r) | (col != c))
        def _():
            kv_copy(m, s).wait_send()

        return carry

    lax.fori_loop(0, members * n, last, 0)

    def sent(i, carry):
        m = lax.div(i, R)
        q = lax.rem(i, R)

        @pl.when(jnp.abs(q - r) <= D)
        def _():
            def one(t, carry):
                @pl.when(jnp.logical_not(tile_place(q, t)[3]))
                def _():
                    g_copy(m, q, t).wait_send()

                return carry

            lax.fori_loop(0, tile_count(q), one, 0)

        return carry

    lax.fori_loop(0, members * R, sent, 0)
    for m in range(members):
        for dist in range(1, D + 1):
            for side in range(2):
                q = r + dist - 2 * dist * side

                @pl.when((q >= 0) & (q < R))
                def _():
                    d_copy(m, dist, side, dist == 1).wait_send()

    for h in range(D):
        for up in (1, 0):
            q, ok = passes(up, h)

            @pl.when(ok)
            def _():
                for m in range(members):
                    for piece in range(PIECES):
                        q_copy(m, q, up, piece).wait_send()
                for kind in range(2):
                    c_copy(q, up, kind).wait_send()

    f_copy(grp, 0, mate).wait_send()
    for k in cousins:
        f_copy(grp, k, mate).wait_send()
        f_copy(grp, groups // 2 + k, mate).wait_send()
    for m in range(members):
        for kind in range(2):
            kv_out(m, kind).wait()
        q_out(m).wait()


def fused(groups, n, heads, blocks, arrays):
    (_, _, hid, dect, base, truth, share, order, q, k, v, lse) = arrays
    C = columns_of(n)
    R = n // C
    D = R // 2
    E = R - 1 - D
    members, rows, width = hid.shape
    chans = base.shape[0]
    bf, f32 = jnp.bfloat16, jnp.float32
    slots = (R + E) * C
    vm = pltpu.VMEM
    dma = pltpu.SemaphoreType.DMA
    scratch = [
        vm(hid.shape, bf),
        vm(dect.shape, bf),
        vm(base.shape, f32),
        vm(truth.shape, f32),
        vm(share.shape, f32),
        vm(order.shape, jnp.int32),
        vm(lse.shape, f32),
        vm(k.shape, bf),
        vm(v.shape, bf),
        vm((groups, members, chans, rows), f32),
        vm((rows, rows), bf),
        vm((members, chans, rows), bf),
        vm((R, members, chans, rows), bf),
        vm((R, members, 2 * heads, rows), f32),
        vm((members, R, rows, width), bf),
        vm((members, n, 2, KB, width), bf),
        vm((members, slots, 2, KB, width), bf),
        vm((members, slots, 2, KB, width), bf),
        vm((members, 2, blocks, KB, width), f32),
        vm((members, rows, width), f32),
        vm((members, width, rows), f32),
        vm((members, max(D - 1, 1), 2, width, rows), f32),
        vm((members, D, 2, width, rows), bf),
        vm((members, max(D - 1, 1), 2, width, rows), bf),
        vm((members, 2, width, rows), bf),
        vm((width, rows), bf),
        vm((width, rows), f32),
        dma((10,)),
        dma((groups,)),
        dma((groups,)),
        dma((members, 2, R, PIECES)),
        dma((members, R, PIECES)),
        dma((2, 2, R)),
        dma((2, R)),
        dma((members, n)),
        dma((members, slots)),
        dma((members, slots)),
        dma((members, n)),
        dma((members, D, 2)),
        dma((members, max(D - 1, 1), 2)),
        dma((members, 2)),
        dma((members, 3)),
    ]
    sums = [(members, rows, width)] + 2 * [(members, blocks, KB, width)]
    held = sum(
        math.prod(x.shape) * jnp.dtype(x.dtype).itemsize
        for x in scratch
        if getattr(x, "memory_space", None) == pltpu.VMEM
    )
    out_bytes = sum(4 * math.prod(x) for x in sums)
    land = (members, n, 2, KB, width)
    near = held + out_bytes + 2 * math.prod(land) + VMEM_SPARE <= VMEM_LIMIT
    if near:
        scratch = [vm(land, bf)] + scratch + [vm((8, 128), bf)]
    else:
        scratch = scratch + [vm((1, 1) + land[2:], bf)]
    limit = VMEM_LIMIT - out_bytes - VMEM_GAP if near else VMEM_LIMIT
    out_type = pltpu.VMEM if near else jax.ShapeDtypeStruct
    smem = pl.BlockSpec(memory_space=pltpu.SMEM)
    anyw = pl.BlockSpec(memory_space=pl.ANY)
    tiles = members * n
    return pl.pallas_call(
        functools.partial(fused_kernel, groups, C, R, heads, near),
        out_shape=[out_type(x, f32) for x in sums]
        + ([] if near else [jax.ShapeDtypeStruct(land, bf)]),
        in_specs=[smem, smem] + [anyw] * 10,
        out_specs=[anyw] * (3 if near else 4),
        scratch_shapes=scratch,
        compiler_params=pltpu.CompilerParams(
            collective_id=0, has_side_effects=True, vmem_limit_bytes=limit
        ),
        cost_estimate=pl.CostEstimate(
            flops=tiles * 10 * rows * KB * width,
            bytes_accessed=16 * 2**20,
            transcendentals=tiles * heads * rows * KB,
        ),
        name="fused",
    )(*arrays), not near


def finish_kernel(staged, *refs):
    arrays = (len(refs) - 2) // (3 if staged else 2)
    stages, read, write = refs[2 * arrays : -2], refs[-2], refs[-1]
    pieces = [(k, m) for m in range(refs[0].shape[0]) for k in range(arrays)]

    def get(k, m):
        return pltpu.make_async_copy(refs[k].at[m], stages[k].at[m], read.at[k, m])

    def put(k, m):
        src = stages[k] if staged else refs[k]
        return pltpu.make_async_copy(src.at[m], refs[arrays + k].at[m], write.at[k, m])

    if staged:
        for piece in pieces:
            get(*piece).start()
    for piece in pieces:
        if staged:
            get(*piece).wait()
        put(*piece).start()
    for piece in pieces:
        put(*piece).wait()


def finish(arrays, staged):
    anyw = pl.BlockSpec(memory_space=pl.ANY)
    sems = pltpu.SemaphoreType.DMA((len(arrays), arrays[0].shape[0]))
    stages = [pltpu.VMEM(x.shape, x.dtype) for x in arrays] if staged else []
    return pl.pallas_call(
        functools.partial(finish_kernel, staged),
        out_shape=[jax.ShapeDtypeStruct(x.shape, x.dtype) for x in arrays],
        in_specs=[anyw] * len(arrays),
        out_specs=[anyw] * len(arrays),
        scratch_shapes=stages + [sems, sems],
        compiler_params=pltpu.CompilerParams(vmem_limit_bytes=(48 if staged else 1) * 2**20),
        cost_estimate=pl.CostEstimate(flops=10**6, bytes_accessed=12 * 2**20, transcendentals=0),
        name="finish",
    )(*arrays)


def shards(
    groups,
    n,
    hidden_embedding,
    decoder_matrix,
    baseline_field,
    truth_field,
    cell_surface_share,
    node_order,
    query,
    key_rows,
    value_rows,
    row_lse,
    kv_owner,
    kv_local,
):
    members, nodes, width = hidden_embedding.shape
    heads = row_lse.shape[1]
    blocks = nodes // KB
    split = (members, blocks, KB, width)
    out, staged = fused(
        groups,
        n,
        heads,
        blocks,
        (
            kv_owner,
            kv_local,
            hidden_embedding,
            decoder_matrix.T,
            baseline_field,
            truth_field,
            cell_surface_share[None],
            node_order,
            query,
            key_rows.reshape(split),
            value_rows.reshape(split),
            row_lse,
        ),
    )
    gq, gk, gv = finish(out[:3], staged)
    return gq, gk.reshape(key_rows.shape), gv.reshape(value_rows.shape)


def solution(mesh):
    rows = P("member", "mesh", None)
    return jax.shard_map(
        functools.partial(shards, mesh.shape["member"], mesh.shape["mesh"]),
        mesh=mesh,
        in_specs=(
            rows,
            P(),
            P(None, "mesh"),
            P(None, "mesh"),
            P("mesh"),
            P("mesh", None),
            rows,
            rows,
            rows,
            P("member", None, "mesh"),
            P(),
            P(),
        ),
        out_specs=(rows, rows, rows),
        check_vma=False,
    )
```

```python
import functools
import math

import jax
import jax.numpy as jnp
from jax import lax
from jax.experimental import pallas as pl
from jax.experimental.pallas import tpu as pltpu
from jax.sharding import PartitionSpec as P

KB = 128
LOSS_SCALE = 4096.0
FAIR_EPS = 0.05
NORM_EPS = 1e-06
PIECES = 2
VMEM_LIMIT = 63 * 2**20
VMEM_SPARE = 2 * 2**20
VMEM_GAP = 2**19
MESH = pl.DeviceIdType.MESH

NN = (((1,), (0,)), ((), ()))
NT = (((1,), (1,)), ((), ()))
TN = (((0,), (0,)), ((), ()))


def dot(a, b, dims):
    return lax.dot_general(a, b, dims, preferred_element_type=jnp.float32)


def unit(d):
    return d * lax.rsqrt(jnp.sum(d * d, axis=0, keepdims=True) + NORM_EPS)


def listed_block(me, owner_ref, local_ref, s):
    found = jnp.int32(0)
    for j in range(owner_ref.shape[1]):
        found = jnp.where(owner_ref[s, j] == me, local_ref[s, j], found)
    return found


def columns_of(n):
    cols = 1
    while (2 * cols) ** 2 <= n and n % (2 * cols) == 0:
        cols *= 2
    return cols


def fused_kernel(
    groups,
    C,
    R,
    heads,
    near,
    owner_ref,
    local_ref,
    hid_in,
    dect_in,
    base_in,
    truth_in,
    share_in,
    order_in,
    q_in,
    k_in,
    v_in,
    lse_in,
    gq_out,
    gk_out,
    gv_out,
    land,
    hid,
    dect,
    base,
    truth,
    share,
    order,
    lse,
    k_vm,
    v_vm,
    fc,
    select,
    deriv,
    cols,
    terms,
    q_buf,
    pick_buf,
    kv_buf,
    kvg,
    kv_sum,
    dq_sum,
    acc,
    part,
    dqs,
    dqr,
    dq_in,
    grads,
    total,
    ld_sem,
    f_snd,
    f_rcv,
    q_snd,
    q_rcv,
    c_snd,
    c_rcv,
    kv_snd,
    kv_rcv,
    g_snd,
    g_rcv,
    d_snd,
    d_rcv,
    l_rcv,
    o_sem,
    stage,
):
    D = R // 2
    E = R - 1 - D
    n = R * C
    members, _, rows, width = q_buf.shape
    dim = width // heads
    pair = 2 * dim
    scale = dim ** (-0.5)
    kb = KB
    me = lax.axis_index("mesh")
    grp = lax.axis_index("member")
    r = lax.div(me, C)
    c = lax.rem(me, C)
    mate = grp + 1 - 2 * lax.rem(grp, 2)
    cousins = range(1, groups // 2)

    def dev(row, col):
        return {"mesh": row * C + col}

    def remote(src, dst, snd, rcv, device):
        return pltpu.make_async_remote_copy(
            src_ref=src, dst_ref=dst, send_sem=snd, recv_sem=rcv, device_id=device, device_id_type=MESH
        )

    loads = [
        (q_in, None),
        (k_in, k_vm),
        (v_in, v_vm),
        (hid_in, hid),
        (dect_in, dect),
        (base_in, base),
        (order_in, order),
        (truth_in, truth),
        (share_in, share),
        (lse_in, lse),
    ]

    def load(i):
        src, dst = loads[i]
        if dst is None:
            dst = q_buf.at[:, r]
        return pltpu.make_async_copy(src, dst, ld_sem.at[i])

    barrier = pltpu.get_barrier_semaphore()

    def greet(device):
        pl.semaphore_signal(barrier, inc=1, device_id=device, device_id_type=MESH)

    greet({"member": mate})
    for k in cousins:
        greet({"member": lax.rem(grp + 2 * k, groups)})
    count = jnp.int32(groups // 2)
    reach = max(1, E)
    for off in range(-reach, reach + 1):
        row = r + off
        ok = (row >= 0) & (row < R)
        for k in range(C):
            if off == 0 and k == 0:
                continue
            col = lax.rem(c + k, C)

            @pl.when(ok)
            def _():
                greet(dev(row, col))

            count = count + jnp.where(ok, 1, 0)

    for i in range(len(loads)):
        load(i).start()

    half = rows // PIECES

    def q_copy(m, q, up, piece):
        ref = q_buf.at[m, q, pl.ds(piece * half, half)]
        return remote(
            ref, ref, q_snd.at[m, up, q, piece], q_rcv.at[m, q, piece], dev(r + (1 if up else -1), c)
        )

    def c_copy(q, up, kind):
        ref = (cols, terms)[kind]
        return remote(
            ref.at[q], ref.at[q], c_snd.at[kind, up, q], c_rcv.at[kind, q], dev(r + (1 if up else -1), c)
        )

    def passes(up, h):
        if up:
            return r - h, (r - h >= 0) & (r + 1 < R)
        return r + h, (r + h < R) & (r - 1 >= 0)

    def send_q(m, h, pieces):
        for piece in pieces:
            for up in (1, 0):
                q, ok = passes(up, h)

                @pl.when(ok)
                def _():
                    if h > 0:
                        q_copy(m, q, up, piece).wait_recv()
                    q_copy(m, q, up, piece).start()

    def send_c(h):
        for up in (1, 0):
            q, ok = passes(up, h)

            @pl.when(ok)
            def _():
                for kind in range(2):
                    if h > 0:
                        c_copy(q, up, kind).wait_recv()
                    c_copy(q, up, kind).start()

    def host_of(s):
        q = lax.div(s, C)
        col = lax.rem(s, C)
        far = jnp.abs(q - r) > D
        row = jnp.where(far, jnp.where(q > r, q - D, q + D), r)
        slot = jnp.where(far, R * C + (jnp.abs(row - r) - 1) * C + c, q * C + c)
        return row, col, slot, far

    def kv_copy(m, s):
        row, col, slot, _ = host_of(s)
        return remote(
            pick_buf.at[m, s], kv_buf.at[m, slot], kv_snd.at[m, s], kv_rcv.at[m, slot], dev(row, col)
        )

    def send_near(m):
        def one(i, carry):
            dist = lax.div(i + 1, 2)
            q = jnp.where(lax.rem(i, 2) == 0, r + dist, r - dist)
            ok = (q >= 0) & (q < R)
            for k in range(1, C):

                @pl.when(ok)
                def _():
                    kv_copy(m, q * C + lax.rem(c + k, C)).start()

            return carry

        lax.fori_loop(0, 2 * D + 1, one, 0)

    def send_far(m, straight):
        def one(q, carry):
            @pl.when(jnp.abs(q - r) > D)
            def _():
                for k in range(0, 1) if straight else range(1, C):
                    kv_copy(m, q * C + lax.rem(c + k, C)).start()

            return carry

        if E > 0:
            lax.fori_loop(0, R, one, 0)

    def f_copy(src, sem, to):
        return remote(fc.at[src], fc.at[src], f_snd.at[sem], f_rcv.at[src], {"member": to})

    def pick(i, carry):
        m = lax.div(i, n)
        s = lax.rem(i, n)
        block = listed_block(me, owner_ref, local_ref, s)
        row, col, slot, _ = host_of(s)
        mine = (row == r) & (col == c)
        key = k_vm[m, block]
        value = v_vm[m, block]

        @pl.when(mine)
        def _():
            kv_buf[m, slot, 0] = key
            kv_buf[m, slot, 1] = value

        @pl.when(jnp.logical_not(mine))
        def _():
            pick_buf[m, s, 0] = key
            pick_buf[m, s, 1] = value

        return carry

    for i in range(1, 3):
        load(i).wait()
    lax.fori_loop(0, n, pick, 0)
    load(0).wait()
    pl.semaphore_wait(barrier, count)
    send_q(0, 0, range(PIECES))
    send_near(0)
    for i in range(3, 6):
        load(i).wait()
    for m in range(members):
        fc[grp, m] = base[...] + dot(dect[...], hid[m], NT)
    for k in cousins:
        f_copy(grp, k, lax.rem(grp + 2 * k, groups)).start()
    f_copy(grp, 0, mate).start()
    send_far(0, True)
    lax.fori_loop(n, members * n, pick, 0)
    for i in range(6, len(loads)):
        load(i).wait()
    select[...] = (
        lax.broadcasted_iota(jnp.int32, (rows, rows), 0) == order[...]
    ).astype(jnp.bfloat16)
    for m in range(members):
        dqs[m, 0, 0] = dot(hid[m], select[...], TN).astype(jnp.bfloat16)
        terms[r, m, pl.ds(0, heads)] = lse[m]

    for h in range(1, D):
        send_q(0, h, range(1))
    for k in cousins:
        src = lax.rem(grp + 2 * k, groups)
        f_copy(src, 0, mate).wait_recv()
        f_copy(src, groups // 2 + k, mate).start()
    for k in range(groups // 2):
        f_copy(lax.rem(mate + 2 * k, groups), 0, mate).wait_recv()

    everyone = members * groups
    lanes_step = 128

    def score(i, carry):
        lanes = pl.ds(pl.multiple_of(i * lanes_step, lanes_step), lanes_step)
        weight = LOSS_SCALE * share[:, lanes]
        for m in range(members):
            own = fc[grp, m, :, lanes]
            couple = jnp.zeros_like(own)
            for other in range(groups):
                for k in range(members):
                    couple = couple + unit(own - fc[other, k, :, lanes])
            polarity = unit(own - truth[:, lanes])
            deriv[m, :, lanes] = (
                weight
                * (polarity / everyone - (1.0 - FAIR_EPS) / (everyone * (everyone - 1)) * couple)
            ).astype(jnp.bfloat16)
        return carry

    lax.fori_loop(0, rows // lanes_step, score, 0)

    def latent(column):
        grads[...] = dot(dect[...], column, TN).astype(jnp.bfloat16)

    for m in range(members):
        column = dot(deriv[m], select[...], NN).astype(jnp.bfloat16)
        cols[r, m] = column
        latent(column)
        for h in range(heads):
            span = pl.ds(h * dim, dim)
            terms[r, m, pl.ds(heads + h, 1)] = jnp.sum(
                grads[span].astype(jnp.float32) * dqs[m, 0, 0, span].astype(jnp.float32),
                axis=0,
                keepdims=True,
            )
    send_c(0)
    for h in range(1, D):
        send_q(0, h, range(1, PIECES))
    send_far(0, False)
    for m in range(1, members):
        send_near(m)

    low = lax.broadcasted_iota(jnp.int32, (kb, pair), 1) < dim

    def tile(m, q, slot):
        for p in range(heads // 2):
            lanes = pl.ds(p * pair, pair)
            key = kv_buf[m, slot, 0, :, lanes]
            value = kv_buf[m, slot, 1, :, lanes]
            nought = jnp.zeros_like(key)
            keys = jnp.concatenate(
                [jnp.where(low, key, nought), jnp.where(low, nought, key)], axis=0
            )
            values = jnp.concatenate(
                [jnp.where(low, value, nought), jnp.where(low, nought, value)], axis=0
            )
            q_pair = q_buf[m, q, :, lanes]
            g_pair = grads[lanes, :]
            scores = dot(keys, q_pair, NT)
            dprobs = dot(values, g_pair, NN)
            prob, dscore = [], []
            for k in range(2):
                span = slice(k * kb, (k + 1) * kb)
                h = 2 * p + k
                pr = jnp.exp(scores[span] * scale - terms[q, m, pl.ds(h, 1), :])
                prob.append(pr.astype(jnp.bfloat16))
                dscore.append(
                    (pr * (dprobs[span] - terms[q, m, pl.ds(heads + h, 1), :])).astype(jnp.bfloat16)
                )
            prob = jnp.concatenate(prob, axis=0)
            dscore = jnp.concatenate(dscore, axis=0)
            dv = dot(prob, g_pair, NT)
            dk = dot(dscore, q_pair, NN) * scale
            kvg[m, slot, 0, :, lanes] = jnp.where(low, dk[:kb], dk[kb:]).astype(jnp.bfloat16)
            kvg[m, slot, 1, :, lanes] = jnp.where(low, dv[:kb], dv[kb:]).astype(jnp.bfloat16)
            total[lanes, :] += dot(keys, dscore, TN)

    def tile_place(q, t):
        turn = lax.div(t, C)
        row = jnp.where(q > r, r - turn, r + turn)
        slot = jnp.where(turn == 0, q * C + t, R * C + t - C)
        return row, lax.rem(t, C), slot, t == c

    def tile_count(q):
        extra = jnp.where(q == r + D, r, jnp.where(q == r - D, R - 1 - r, 0))
        return C * (1 + extra)

    def g_copy(m, q, t):
        row, col, slot, _ = tile_place(q, t)
        return remote(
            kvg.at[m, slot],
            land.at[m, q * C + c],
            g_snd.at[m, slot],
            g_rcv.at[m, q * C + c],
            dev(row, col),
        )

    def kv_arrival(m, slot):
        return remote(
            pick_buf.at[0, 0], kv_buf.at[m, slot], kv_snd.at[0, 0], kv_rcv.at[m, slot], dev(r, c)
        )

    def d_copy(m, dist, side, last):
        src, snd = dqs.at[m, dist - 1, side], d_snd.at[m, dist - 1, side]
        device = dev(r + 1 - 2 * side, c)
        if last:
            return remote(src, dq_in.at[m, side], snd, l_rcv.at[m, side], device)
        return remote(src, dqr.at[m, dist - 2, side], snd, d_rcv.at[m, dist - 2, side], device)

    plan = [(0, 0)] + [(0, d) for d in range(1, D)]
    plan += [(m, 0) for m in range(1, members)] + [(0, D)]
    relay_at = len(plan)
    for m in range(1, members):
        plan += [(m, d) for d in range(1, D + 1)]

    def table(step, values):
        found = jnp.int32(values[0])
        for k, value in enumerate(values):
            found = jnp.where(step == k, jnp.int32(value), found)
        return found

    def job(i, carry):
        step = lax.div(i, 2)
        side = lax.rem(i, 2)
        m = table(step, [a for a, _ in plan])
        dist = table(step, [b for _, b in plan])
        q = r + dist - 2 * dist * side
        ok = (q >= 0) & (q < R) & ((dist > 0) | (side == 0))

        @pl.when(i == 2)
        def _():
            for h in range(1, D):
                send_c(h)
            for k in range(1, members):
                send_q(k, 0, range(PIECES))
            for k in range(1, members):
                send_far(k, True)
                send_far(k, False)

        @pl.when(i == 2 * (relay_at - 1))
        def _():
            for k in range(1, 2):
                for h in range(1, min(D, 2)):
                    send_q(k, h, range(1))

        @pl.when(i == 2 * relay_at)
        def _():
            for k in range(1, members):
                for h in range(1, D):
                    send_q(k, h, range(1 if k == 1 and h == 1 else 0, PIECES))
            for far_side in range(2):
                far_q = r + D - 2 * D * far_side

                @pl.when((far_q >= 0) & (far_q < R))
                def _():
                    d_copy(0, D, far_side, D == 1).start()

                    def late(t, carry):
                        g_copy(0, far_q, t).start()
                        return carry

                    lax.fori_loop(C, tile_count(far_q), late, 0)

        @pl.when(ok)
        def _():
            for up in (1, 0):
                edge = (r == R - 1) if up else (r == 0)
                here = ((q < r) if up else (q > r)) & ((dist == D) | edge)

                @pl.when(here)
                def _():
                    for piece in range(PIECES):
                        q_copy(m, q, up, piece).wait_recv()

                    @pl.when(m == 0)
                    def _():
                        c_copy(q, up, 0).wait_recv()
                        c_copy(q, up, 1).wait_recv()

            latent(cols[q, m])
            total[...] = jnp.zeros_like(total)

            def one(t, carry):
                _, _, slot, mine = tile_place(q, t)

                @pl.when(jnp.logical_not(mine))
                def _():
                    kv_arrival(m, slot).wait_recv()

                tile(m, q, slot)

                @pl.when(jnp.logical_not(mine) & ((t < C) | (m > 0)))
                def _():
                    g_copy(m, q, t).start()

                return carry

            lax.fori_loop(0, tile_count(q), one, 0)

            @pl.when(dist == 0)
            def _():
                acc[m] = total[...] * scale

            @pl.when((dist > 0) & (dist < D))
            def _():
                part[m, jnp.minimum(jnp.maximum(dist - 1, 0), max(D - 2, 0)), side] = total[...] * scale

            @pl.when(dist == D)
            def _():
                dqs[m, D - 1, side] = (total[...] * scale).astype(jnp.bfloat16)

                @pl.when(m > 0)
                def _():
                    d_copy(m, D, side, D == 1).start()

        return carry

    lax.fori_loop(0, 2 * len(plan), job, 0)

    for m in range(members):
        for dist in range(D - 1, 0, -1):
            for side in range(2):
                q = r + dist - 2 * dist * side
                chained = (r > 0) if side == 0 else (r < R - 1)
                ok = (q >= 0) & (q < R)

                @pl.when(ok & chained)
                def _():
                    d_copy(m, dist + 1, side, False).wait_recv()
                    dqs[m, dist - 1, side] = (
                        part[m, dist - 1, side] + dqr[m, dist - 1, side].astype(jnp.float32)
                    ).astype(jnp.bfloat16)

                @pl.when(ok & jnp.logical_not(chained))
                def _():
                    dqs[m, dist - 1, side] = part[m, dist - 1, side].astype(jnp.bfloat16)

                @pl.when(ok)
                def _():
                    d_copy(m, dist, side, dist == 1).start()

    def kv_out(m, kind):
        return pltpu.make_async_copy(kv_sum.at[m, kind], (gk_out, gv_out)[kind].at[m], o_sem.at[m, kind])

    def q_out(m):
        return pltpu.make_async_copy(dq_sum.at[m], gq_out.at[m], o_sem.at[m, 2])

    def landed(ref, m, s, col, row):
        return remote(kvg.at[0, 0], ref, g_snd.at[0, 0], g_rcv.at[m, s], dev(row, col))

    chunk = 32

    def gather(m):
        kv_sum[m] = jnp.zeros_like(kv_sum[m])

        def one(i, carry):
            dist = lax.div(i, 2 * C)
            side = lax.rem(lax.div(i, C), 2)
            q = r + dist - 2 * dist * side
            ok = (q >= 0) & (q < R) & ((dist > 0) | (side == 0))

            @pl.when(ok)
            def _():
                s = q * C + lax.rem(i, C)
                row, col, slot, _ = host_of(s)
                mine = (row == r) & (col == c)
                block = listed_block(me, owner_ref, local_ref, s)

                def add(ref, a, b):
                    def rows_of(j, carry):
                        span = pl.ds(pl.multiple_of(j * chunk, chunk), chunk)
                        for kind in range(2):
                            value = ref[a, b, kind, span].astype(jnp.float32)
                            for k in range(kv_sum.shape[2]):
                                kv_sum[m, kind, k, span] += jnp.where(block == k, value, 0.0)
                        return carry

                    lax.fori_loop(0, kb // chunk, rows_of, 0)

                @pl.when(mine)
                def _():
                    add(kvg, m, slot)

                @pl.when(jnp.logical_not(mine))
                def _():
                    landed(land.at[m, s], m, s, col, row).wait_recv()
                    if near:
                        add(land, m, s)
                    else:
                        bring = pltpu.make_async_copy(land.at[m, s], stage.at[0, 0], ld_sem.at[0])
                        bring.start()
                        bring.wait()
                        add(stage, 0, 0)

            return carry

        lax.fori_loop(0, 2 * C * R, one, 0)
        for kind in range(2):
            kv_out(m, kind).start()

    def settle(m):
        for side in range(2):
            @pl.when((r > 0) if side == 0 else (r < R - 1))
            def _():
                d_copy(m, 1, side, True).wait_recv()
                acc[m] = acc[m] + dq_in[m, side].astype(jnp.float32)
        dq_sum[m] = acc[m].T
        q_out(m).start()

    for m in range(members - 1):
        gather(m)
        settle(m)
    def last(i, carry):
        m = lax.div(i, n)
        s = lax.rem(i, n)
        row, col, _, _ = host_of(s)

        @pl.when((row != r) | (col != c))
        def _():
            kv_copy(m, s).wait_send()

        return carry

    lax.fori_loop(0, members * n, last, 0)
    gather(members - 1)
    settle(members - 1)

    def sent(i, carry):
        m = lax.div(i, R)
        q = lax.rem(i, R)

        @pl.when(jnp.abs(q - r) <= D)
        def _():
            def one(t, carry):
                @pl.when(jnp.logical_not(tile_place(q, t)[3]))
                def _():
                    g_copy(m, q, t).wait_send()

                return carry

            lax.fori_loop(0, tile_count(q), one, 0)

        return carry

    lax.fori_loop(0, members * R, sent, 0)
    for m in range(members):
        for dist in range(1, D + 1):
            for side in range(2):
                q = r + dist - 2 * dist * side

                @pl.when((q >= 0) & (q < R))
                def _():
                    d_copy(m, dist, side, dist == 1).wait_send()

    for h in range(D):
        for up in (1, 0):
            q, ok = passes(up, h)

            @pl.when(ok)
            def _():
                for m in range(members):
                    for piece in range(PIECES):
                        q_copy(m, q, up, piece).wait_send()
                for kind in range(2):
                    c_copy(q, up, kind).wait_send()

    f_copy(grp, 0, mate).wait_send()
    for k in cousins:
        f_copy(grp, k, mate).wait_send()
        f_copy(grp, groups // 2 + k, mate).wait_send()
    for m in range(members):
        for kind in range(2):
            kv_out(m, kind).wait()
        q_out(m).wait()


def fused(groups, n, heads, blocks, arrays):
    (_, _, hid, dect, base, truth, share, order, q, k, v, lse) = arrays
    C = columns_of(n)
    R = n // C
    D = R // 2
    E = R - 1 - D
    members, rows, width = hid.shape
    chans = base.shape[0]
    bf, f32 = jnp.bfloat16, jnp.float32
    slots = (R + E) * C
    vm = pltpu.VMEM
    dma = pltpu.SemaphoreType.DMA
    scratch = [
        vm(hid.shape, bf),
        vm(dect.shape, bf),
        vm(base.shape, f32),
        vm(truth.shape, f32),
        vm(share.shape, f32),
        vm(order.shape, jnp.int32),
        vm(lse.shape, f32),
        vm(k.shape, bf),
        vm(v.shape, bf),
        vm((groups, members, chans, rows), f32),
        vm((rows, rows), bf),
        vm((members, chans, rows), bf),
        vm((R, members, chans, rows), bf),
        vm((R, members, 2 * heads, rows), f32),
        vm((members, R, rows, width), bf),
        vm((members, n, 2, KB, width), bf),
        vm((members, slots, 2, KB, width), bf),
        vm((members, slots, 2, KB, width), bf),
        vm((members, 2, blocks, KB, width), f32),
        vm((members, rows, width), f32),
        vm((members, width, rows), f32),
        vm((members, max(D - 1, 1), 2, width, rows), f32),
        vm((members, D, 2, width, rows), bf),
        vm((members, max(D - 1, 1), 2, width, rows), bf),
        vm((members, 2, width, rows), bf),
        vm((width, rows), bf),
        vm((width, rows), f32),
        dma((10,)),
        dma((groups,)),
        dma((groups,)),
        dma((members, 2, R, PIECES)),
        dma((members, R, PIECES)),
        dma((2, 2, R)),
        dma((2, R)),
        dma((members, n)),
        dma((members, slots)),
        dma((members, slots)),
        dma((members, n)),
        dma((members, D, 2)),
        dma((members, max(D - 1, 1), 2)),
        dma((members, 2)),
        dma((members, 3)),
    ]
    sums = [(members, rows, width)] + 2 * [(members, blocks, KB, width)]
    held = sum(
        math.prod(x.shape) * jnp.dtype(x.dtype).itemsize
        for x in scratch
        if getattr(x, "memory_space", None) == pltpu.VMEM
    )
    out_bytes = sum(4 * math.prod(x) for x in sums)
    land = (members, n, 2, KB, width)
    near = held + out_bytes + 2 * math.prod(land) + VMEM_SPARE <= VMEM_LIMIT
    if near:
        scratch = [vm(land, bf)] + scratch + [vm((8, 128), bf)]
    else:
        scratch = scratch + [vm((1, 1) + land[2:], bf)]
    limit = VMEM_LIMIT - out_bytes - VMEM_GAP if near else VMEM_LIMIT
    out_type = pltpu.VMEM if near else jax.ShapeDtypeStruct
    smem = pl.BlockSpec(memory_space=pltpu.SMEM)
    anyw = pl.BlockSpec(memory_space=pl.ANY)
    tiles = members * n
    return pl.pallas_call(
        functools.partial(fused_kernel, groups, C, R, heads, near),
        out_shape=[out_type(x, f32) for x in sums]
        + ([] if near else [jax.ShapeDtypeStruct(land, bf)]),
        in_specs=[smem, smem] + [anyw] * 10,
        out_specs=[anyw] * (3 if near else 4),
        scratch_shapes=scratch,
        compiler_params=pltpu.CompilerParams(
            collective_id=0, has_side_effects=True, vmem_limit_bytes=limit
        ),
        cost_estimate=pl.CostEstimate(
            flops=tiles * 10 * rows * KB * width,
            bytes_accessed=16 * 2**20,
            transcendentals=tiles * heads * rows * KB,
        ),
        name="fused",
    )(*arrays), not near


def finish_kernel(staged, *refs):
    arrays = (len(refs) - 2) // (3 if staged else 2)
    stages, read, write = refs[2 * arrays : -2], refs[-2], refs[-1]
    pieces = [(k, m) for m in range(refs[0].shape[0]) for k in range(arrays)]

    def get(k, m):
        return pltpu.make_async_copy(refs[k].at[m], stages[k].at[m], read.at[k, m])

    def put(k, m):
        src = stages[k] if staged else refs[k]
        return pltpu.make_async_copy(src.at[m], refs[arrays + k].at[m], write.at[k, m])

    if staged:
        for piece in pieces:
            get(*piece).start()
    for piece in pieces:
        if staged:
            get(*piece).wait()
        put(*piece).start()
    for piece in pieces:
        put(*piece).wait()


def finish(arrays, staged):
    anyw = pl.BlockSpec(memory_space=pl.ANY)
    sems = pltpu.SemaphoreType.DMA((len(arrays), arrays[0].shape[0]))
    stages = [pltpu.VMEM(x.shape, x.dtype) for x in arrays] if staged else []
    return pl.pallas_call(
        functools.partial(finish_kernel, staged),
        out_shape=[jax.ShapeDtypeStruct(x.shape, x.dtype) for x in arrays],
        in_specs=[anyw] * len(arrays),
        out_specs=[anyw] * len(arrays),
        scratch_shapes=stages + [sems, sems],
        compiler_params=pltpu.CompilerParams(vmem_limit_bytes=(48 if staged else 1) * 2**20),
        cost_estimate=pl.CostEstimate(flops=10**6, bytes_accessed=12 * 2**20, transcendentals=0),
        name="finish",
    )(*arrays)


def shards(
    groups,
    n,
    hidden_embedding,
    decoder_matrix,
    baseline_field,
    truth_field,
    cell_surface_share,
    node_order,
    query,
    key_rows,
    value_rows,
    row_lse,
    kv_owner,
    kv_local,
):
    members, nodes, width = hidden_embedding.shape
    heads = row_lse.shape[1]
    blocks = nodes // KB
    split = (members, blocks, KB, width)
    out, staged = fused(
        groups,
        n,
        heads,
        blocks,
        (
            kv_owner,
            kv_local,
            hidden_embedding,
            decoder_matrix.T,
            baseline_field,
            truth_field,
            cell_surface_share[None],
            node_order,
            query,
            key_rows.reshape(split),
            value_rows.reshape(split),
            row_lse,
        ),
    )
    gq, gk, gv = finish(out[:3], staged)
    return gq, gk.reshape(key_rows.shape), gv.reshape(value_rows.shape)


def solution(mesh):
    rows = P("member", "mesh", None)
    return jax.shard_map(
        functools.partial(shards, mesh.shape["member"], mesh.shape["mesh"]),
        mesh=mesh,
        in_specs=(
            rows,
            P(),
            P(None, "mesh"),
            P(None, "mesh"),
            P("mesh"),
            P("mesh", None),
            rows,
            rows,
            rows,
            P("member", None, "mesh"),
            P(),
            P(),
        ),
        out_specs=(rows, rows, rows),
        check_vma=False,
    )
```
